512 devices in a mesh: layer: 16 (over y, core), row: 4 (over x), col: 8 (over z).
Axes of the slice: x: 4, y: 8, z: 8, core: 2. Of those that a mesh axis runs over, the one named last changes fastest.
Arguments:
- left: float32 [2048, 4096], P('row', ('layer', 'col')), may hold values from -6 to 6
- right: float32 [4096, 32768], P(('layer', 'row'), 'col'), may hold values from -0.09375 to 0.09375
Outputs:
- product: float32 [2048, 32768], P(('row', 'layer'), 'col')
The draws below stay inside these ranges and needn't reach their ends.
All inputs are finite; a program needn't handle non-finite values.
Results may differ from the reference program's by a relative error of at most 0.000076.
Values sent between devices are 32-bit elements; how exact they have to be, the bound alone decides.
No kernel may reach another device: no remote copies, remote signals or barrier semaphores. Data moves between devices by JAX's collectives and lax.ppermute only.
A program may use at most 128 MiB of HBM per device.

```python
import jax
import jax.numpy as jnp
from jax import lax

NCOLS = 32768
K = 4096
M = 2048


def block_scale(key, dims, cuts, low, top_value):
    loudness = 1.0
    for position, parts in cuts:
        steps = jax.random.uniform(jax.random.fold_in(jax.random.fold_in(key, 6), position), (parts,), jnp.float32, low / len(cuts), top_value / len(cuts))
        loudness = loudness * jnp.repeat(jnp.exp(steps), dims[position] // parts).reshape((-1,) + (1,) * (len(dims) - 1 - position))
    return loudness


def bell_draw(stream_key, dims, width, limit, split=(), dtype=jnp.bfloat16):
    array = width * jax.random.normal(stream_key, dims, jnp.float32)
    if split:
        array = array * block_scale(stream_key, dims, split, -0.22, 0.18)
    return jnp.clip(array, -limit, limit).astype(dtype)


def setup_inputs(seed: int = 0) -> dict:
    key_list = jax.random.split(jax.random.key(seed), 3)
    return {
        "left": bell_draw(key_list[0], (M, K), 1.0, 6.0, ((0, 4), (1, 128)), jnp.float32),
        "right": bell_draw(key_list[1], (K, NCOLS), K ** -0.5, 0.09375, ((0, 64), (1, 8)), jnp.float32),
    }


def reference(left, right):
    return jnp.dot(left, right, precision=lax.Precision.HIGHEST, preferred_element_type=jnp.float32)
```

```python
import jax
import jax.numpy as jnp
from jax import lax
from jax.sharding import PartitionSpec as P


def dot(a, b):
    return lax.dot_general(
        a,
        b,
        (((0,), (0,)), ((), ())),
        precision=lax.Precision.HIGH,
        preferred_element_type=jnp.float32,
    )


def body(left, right):
    layers, rows = lax.axis_size("layer"), lax.axis_size("row")
    cols = lax.axis_size("col")
    ys = layers // 2
    layer, x = lax.axis_index("layer"), lax.axis_index("row")
    y, c = layer // 2, layer % 2
    n = x % 2
    width = right.shape[1] // 2
    depth = left.shape[1]
    height = left.shape[0] // layers

    swap_core = [(i, i ^ 1) for i in range(layers)]
    swap_pair = [(i, i ^ 1) for i in range(rows)]
    swap_both = [
        (i * rows + j, (i ^ 1) * rows + (j ^ 1))
        for i in range(layers)
        for j in range(rows)
    ]
    onward = [(2 * i, 2 * ((i + 1) % ys)) for i in range(ys)]
    onward += [(2 * i + 1, 2 * ((i - 1) % ys) + 1) for i in range(ys)]

    def block_of(slot, core):
        away = jnp.where(slot == 0, 4, jnp.where(slot == 7, 0, 3 - (slot - 1) // 2))
        half = jnp.where((slot == 0) | (slot == 7), core, core ^ ((slot + 1) % 2))
        return ((y + (1 - 2 * core) * away) % ys) * 2 + half

    slots = 8
    count = slots * height
    lane = lax.broadcasted_iota(jnp.int32, (left.shape[0], 2 * count), 1)
    source = lax.broadcasted_iota(jnp.int32, (left.shape[0], 2 * count), 0)
    core = jnp.where(lane < count, c, 1 - c)
    slot = (lane // height) % slots
    wanted = block_of(slot, core) * height + lane % height
    picked = lax.dot_general(
        left,
        (source == wanted).astype(jnp.float32),
        (((0,), (0,)), ((), ())),
        precision=lax.Precision.HIGHEST,
    )
    mine, theirs = picked[:, :count], picked[:, count:]
    both = jnp.concatenate([mine, lax.ppermute(theirs, "layer", swap_core)], 0)

    keep = lax.dynamic_slice_in_dim(right, n * width, width, 1)
    give = lax.dynamic_slice_in_dim(right, (1 - n) * width, width, 1)
    step = [(i, (i + 1) % rows) for i in range(rows)]
    from_low = lax.ppermute(give, "row", step)
    from_high = lax.ppermute(give, "row", [(j, i) for i, j in step])
    from_far = lax.ppermute(keep, "row", [(i, (i + 2) % rows) for i in range(rows)])
    own_b = jnp.concatenate([keep, from_low, from_high, from_far], 0)
    other_b = lax.ppermute(own_b, "layer", swap_core)

    spread = jnp.broadcast_to(both[None], (cols,) + both.shape)
    full = lax.all_to_all(spread, "col", split_axis=0, concat_axis=0, tiled=True)
    full = full.reshape(rows, cols // rows, 2, depth, count)

    def ordered(part, at):
        order = [at, at - 1, at + 1, at + 2]
        part = jnp.stack(
            [lax.dynamic_index_in_dim(part, i % rows, 0, keepdims=False) for i in order]
        )
        part = part.transpose(2, 0, 1, 3, 4)
        return part.reshape(2, cols * depth, part.shape[-1])

    first = 3 * height
    early, late = full[..., :first], full[..., first:]
    early_pair = lax.ppermute(ordered(early, x ^ 1), "row", swap_pair)
    late_pair = lax.ppermute(ordered(late, x ^ 1), "row", swap_pair)
    early, late = ordered(early, x), ordered(late, x)

    def product(a):
        return dot(a[0], own_b) + dot(a[1], other_b)

    def reduce(near, far):
        near_p = product(near)
        total = lax.ppermute(near_p[:height], "layer", onward)
        total = jnp.concatenate(
            [near_p[height : 2 * height] + total, near_p[2 * height :]], 0
        )
        far_p = product(far)
        total = lax.ppermute(total, "layer", onward)
        total = lax.ppermute(total + far_p[: 2 * height], "layer", onward)
        total = lax.ppermute(total + far_p[2 * height : 4 * height], "layer", onward)
        return total[:height] + far_p[4 * height :], total[height:]

    self_own, self_other = reduce(early, late)
    pair_own, pair_other = reduce(early_pair, late_pair)
    in_core = lax.ppermute(self_other, "layer", swap_core)
    in_pair = lax.ppermute(pair_own, "row", swap_pair)
    in_both = lax.ppermute(pair_other, ("layer", "row"), swap_both)
    here = self_own + in_core
    there = in_pair + in_both
    return jnp.concatenate(
        [jnp.where(n == 0, here, there), jnp.where(n == 0, there, here)], 1
    )


def solution(mesh):
    in_specs = (P("row", ("layer", "col")), P(("layer", "row"), "col"))
    out_specs = P(("row", "layer"), "col")
    return jax.shard_map(
        body, mesh=mesh, in_specs=in_specs, out_specs=out_specs, check_vma=False
    )
```

```python
import jax
import jax.numpy as jnp
from jax import lax
from jax.sharding import PartitionSpec as P


def dot(a, b):
    return lax.dot_general(
        a,
        b,
        (((0,), (0,)), ((), ())),
        precision=lax.Precision.HIGH,
        preferred_element_type=jnp.float32,
    )


def body(left, right):
    layers, rows = lax.axis_size("layer"), lax.axis_size("row")
    cols = lax.axis_size("col")
    ys = layers // 2
    layer, x = lax.axis_index("layer"), lax.axis_index("row")
    y, c = layer // 2, layer % 2
    n = x % 2
    width = right.shape[1] // 2
    depth = left.shape[1]
    height = left.shape[0] // layers

    swap_core = [(i, i ^ 1) for i in range(layers)]
    swap_pair = [(i, i ^ 1) for i in range(rows)]
    onward = [(2 * i, 2 * ((i + 1) % ys)) for i in range(ys)]
    onward += [(2 * i + 1, 2 * ((i - 1) % ys) + 1) for i in range(ys)]
    onward_cross = [(i, j ^ 1) for i, j in onward]

    def joint(pairs):
        return [(i * rows + k, j * rows + (k ^ 1)) for i, j in pairs for k in range(rows)]


    def block_of(slot, core):
        away = jnp.where(slot == 0, 4, jnp.where(slot == 7, 0, 3 - (slot - 1) // 2))
        half = jnp.where((slot == 0) | (slot == 7), core, core ^ ((slot + 1) % 2))
        return ((y + (1 - 2 * core) * away) % ys) * 2 + half

    slots = 8
    quarter = slots * height // 2
    lane = lax.broadcasted_iota(jnp.int32, (left.shape[0], 4 * quarter), 1)
    source = lax.broadcasted_iota(jnp.int32, (left.shape[0], 4 * quarter), 0)
    core = jnp.where((lane // quarter) % 2 == 0, c, 1 - c)
    slot = (lane // (2 * quarter)) * (slots // 2) + (lane % quarter) // height
    wanted = block_of(slot, core) * height + lane % height
    picked = lax.dot_general(
        left,
        (source == wanted).astype(jnp.float32),
        (((0,), (0,)), ((), ())),
        precision=lax.Precision.HIGHEST,
    )

    keep = lax.dynamic_slice_in_dim(right, n * width, width, 1)
    give = lax.dynamic_slice_in_dim(right, (1 - n) * width, width, 1)
    step = [(i, (i + 1) % rows) for i in range(rows)]
    from_low = lax.ppermute(give, "row", step)
    from_high = lax.ppermute(give, "row", [(j, i) for i, j in step])
    from_far = lax.ppermute(keep, "row", [(i, (i + 2) % rows) for i in range(rows)])
    own_b = jnp.concatenate([keep, from_far, from_high, from_low], 0)

    spread = jnp.broadcast_to(picked[None], (cols,) + picked.shape)
    full = lax.all_to_all(spread, "col", split_axis=0, concat_axis=0, tiled=True)
    full = full.reshape(rows, cols // rows * depth, 4 * quarter)

    def ordered(part, at):
        order = [at, at + 2, at + 1, at - 1]
        return jnp.concatenate(
            [lax.dynamic_index_in_dim(part, i % rows, 0, keepdims=False) for i in order],
            0,
        )

    near_a, far_a = full[..., : 2 * quarter], full[..., 2 * quarter :]
    near_pair = lax.ppermute(ordered(near_a, x ^ 1), "row", swap_pair)
    far_pair = lax.ppermute(ordered(far_a, x ^ 1), "row", swap_pair)
    near_a, far_a = ordered(near_a, x), ordered(far_a, x)

    def product(a):
        part = dot(a, own_b)
        other = part[quarter:]
        return part[:quarter] + lax.ppermute(other, "layer", swap_core)

    def reduce(near, far):
        near_p = product(near)
        total = lax.ppermute(near_p[:height], "layer", onward)
        total = jnp.concatenate(
            [near_p[height : 2 * height] + total, near_p[2 * height : 3 * height]], 0
        )
        far_p = product(far)
        total = lax.ppermute(total, "layer", onward)
        total = jnp.concatenate(
            [
                total[:height] + near_p[3 * height :],
                total[height:] + far_p[:height],
            ],
            0,
        )
        total = lax.ppermute(total, "layer", onward)
        total = total + far_p[height : 3 * height]
        return total[:height], total[height:], far_p[3 * height :]

    same, cross, here = reduce(near_a, far_a)
    here = here + lax.ppermute(same, "layer", onward)
    here = here + lax.ppermute(cross, "layer", onward_cross)
    same, cross, there = reduce(near_pair, far_pair)
    there = lax.ppermute(there, "row", swap_pair)
    there = there + lax.ppermute(same, ("layer", "row"), joint(onward))
    there = there + lax.ppermute(cross, ("layer", "row"), joint(onward_cross))
    return jnp.concatenate(
        [jnp.where(n == 0, here, there), jnp.where(n == 0, there, here)], 1
    )


def solution(mesh):
    in_specs = (P("row", ("layer", "col")), P(("layer", "row"), "col"))
    out_specs = P(("row", "layer"), "col")
    return jax.shard_map(
        body, mesh=mesh, in_specs=in_specs, out_specs=out_specs, check_vma=False
    )
```

```python
import jax
import jax.numpy as jnp
from jax import lax
from jax.sharding import PartitionSpec as P


def dot(a, b):
    return lax.dot_general(
        a,
        b,
        (((0,), (0,)), ((), ())),
        precision=lax.Precision.HIGH,
        preferred_element_type=jnp.float32,
    )


def body(left, right):
    layers, rows = lax.axis_size("layer"), lax.axis_size("row")
    cols = lax.axis_size("col")
    ys = layers // 2
    layer, x = lax.axis_index("layer"), lax.axis_index("row")
    y, c = layer // 2, layer % 2
    n = x % 2
    width = right.shape[1] // 2
    depth = left.shape[1]
    height = left.shape[0] // layers

    swap_core = [(i, i ^ 1) for i in range(layers)]
    swap_pair = [(i, i ^ 1) for i in range(rows)]
    onward = [(2 * i, 2 * ((i + 1) % ys)) for i in range(ys)]
    onward += [(2 * i + 1, 2 * ((i - 1) % ys) + 1) for i in range(ys)]
    onward_cross = [(i, j ^ 1) for i, j in onward]

    def joint(pairs):
        return [(i * rows + k, j * rows + (k ^ 1)) for i, j in pairs for k in range(rows)]


    def block_of(slot, core):
        away = jnp.where(slot == 0, 4, jnp.where(slot == 7, 0, 3 - (slot - 1) // 2))
        half = jnp.where((slot == 0) | (slot == 7), core, core ^ ((slot + 1) % 2))
        return ((y + (1 - 2 * core) * away) % ys) * 2 + half

    close, distant = 3 * height, 5 * height
    count = 2 * (close + distant)
    lane = lax.broadcasted_iota(jnp.int32, (left.shape[0], count), 1)
    source = lax.broadcasted_iota(jnp.int32, (left.shape[0], count), 0)
    late = lane >= 2 * close
    place = jnp.where(late, lane - 2 * close, lane)
    size = jnp.where(late, distant, close)
    second = (place >= size).astype(jnp.int32)
    core = c ^ second
    slot = jnp.where(late, 3, 0) + (place - second * size) // height
    wanted = block_of(slot, core) * height + lane % height
    picked = lax.dot_general(
        left,
        (source == wanted).astype(jnp.float32),
        (((0,), (0,)), ((), ())),
        precision=lax.Precision.HIGHEST,
    )

    keep = lax.dynamic_slice_in_dim(right, n * width, width, 1)
    give = lax.dynamic_slice_in_dim(right, (1 - n) * width, width, 1)
    step = [(i, (i + 1) % rows) for i in range(rows)]
    from_low = lax.ppermute(give, "row", step)
    from_high = lax.ppermute(give, "row", [(j, i) for i, j in step])
    from_far = lax.ppermute(keep, "row", [(i, (i + 2) % rows) for i in range(rows)])
    own_b = jnp.concatenate([keep, from_far, from_high, from_low], 0)

    spread = jnp.broadcast_to(picked[None], (cols,) + picked.shape)
    full = lax.all_to_all(spread, "col", split_axis=0, concat_axis=0, tiled=True)
    full = full.reshape(rows, cols // rows * depth, count)

    def ordered(part, at):
        order = [at, at + 2, at + 1, at - 1]
        return jnp.concatenate(
            [lax.dynamic_index_in_dim(part, i % rows, 0, keepdims=False) for i in order],
            0,
        )

    near_a, far_a = full[..., : 2 * close], full[..., 2 * close :]
    near_pair = lax.ppermute(ordered(near_a, x ^ 1), "row", swap_pair)
    far_pair = lax.ppermute(ordered(far_a, x ^ 1), "row", swap_pair)
    near_a, far_a = ordered(near_a, x), ordered(far_a, x)

    def product(a):
        part = dot(a, own_b)
        other = part[close:]
        return part[:close] + lax.ppermute(other, "layer", swap_core)

    part = dot(jnp.concatenate([far_a, far_pair], 1), own_b)
    part = part.reshape(4, distant, width)
    other = jnp.concatenate([part[1], part[3]], 0)
    other = lax.ppermute(other, "layer", swap_core)
    own_far, pair_far = part[0] + other[:distant], part[2] + other[distant:]

    def reduce(near, far_p):
        near_p = product(near)
        total = lax.ppermute(near_p[:height], "layer", onward)
        total = jnp.concatenate(
            [near_p[height : 2 * height] + total, near_p[2 * height :]], 0
        )
        total = lax.ppermute(total, "layer", onward)
        total = lax.ppermute(total + far_p[: 2 * height], "layer", onward)
        total = total + far_p[2 * height : 4 * height]
        return total[:height], total[height:], far_p[4 * height :]

    same, cross, here = reduce(near_a, own_far)
    here = here + lax.ppermute(same, "layer", onward)
    here = here + lax.ppermute(cross, "layer", onward_cross)
    same, cross, there = reduce(near_pair, pair_far)
    there = lax.ppermute(there, "row", swap_pair)
    total = jnp.concatenate([same, cross], 0)
    total = lax.ppermute(total, ("layer", "row"), joint(onward))
    there = there + total[:height] + lax.ppermute(total[height:], "layer", swap_core)
    return jnp.concatenate(
        [jnp.where(n == 0, here, there), jnp.where(n == 0, there, here)], 1
    )


def solution(mesh):
    in_specs = (P("row", ("layer", "col")), P(("layer", "row"), "col"))
    out_specs = P(("row", "layer"), "col")
    return jax.shard_map(
        body, mesh=mesh, in_specs=in_specs, out_specs=out_specs, check_vma=False
    )
```

```python
import jax
import jax.numpy as jnp
from jax import lax
from jax.sharding import PartitionSpec as P


def dot(a, b):
    return lax.dot_general(
        a,
        b,
        (((0,), (0,)), ((), ())),
        precision=lax.Precision.HIGH,
        preferred_element_type=jnp.float32,
    )


def body(left, right):
    layers, rows = lax.axis_size("layer"), lax.axis_size("row")
    cols = lax.axis_size("col")
    ys = layers // 2
    layer, x = lax.axis_index("layer"), lax.axis_index("row")
    y, c = layer // 2, layer % 2
    n = x % 2
    width = right.shape[1] // 2
    depth = left.shape[1]
    height = left.shape[0] // layers

    swap_core = [(i, i ^ 1) for i in range(layers)]
    swap_pair = [(i, i ^ 1) for i in range(rows)]
    onward = [(2 * i, 2 * ((i + 1) % ys)) for i in range(ys)]
    onward += [(2 * i + 1, 2 * ((i - 1) % ys) + 1) for i in range(ys)]

    def joint(pairs):
        return [(i * rows + k, j * rows + (k ^ 1)) for i, j in pairs for k in range(rows)]


    def block_of(slot, core):
        away = jnp.where(slot == 0, 4, jnp.where(slot == 7, 0, 3 - (slot - 1) // 2))
        half = jnp.where((slot == 0) | (slot == 7), core, core ^ ((slot + 1) % 2))
        return ((y + (1 - 2 * core) * away) % ys) * 2 + half

    close, distant = 3 * height, 5 * height
    count = 2 * (close + distant)
    lane = lax.broadcasted_iota(jnp.int32, (left.shape[0], count), 1)
    source = lax.broadcasted_iota(jnp.int32, (left.shape[0], count), 0)
    late = lane >= 2 * close
    place = jnp.where(late, lane - 2 * close, lane)
    size = jnp.where(late, distant, close)
    second = (place >= size).astype(jnp.int32)
    core = c ^ second
    slot = jnp.where(late, 3, 0) + (place - second * size) // height
    wanted = block_of(slot, core) * height + lane % height
    picked = lax.dot_general(
        left,
        (source == wanted).astype(jnp.float32),
        (((0,), (0,)), ((), ())),
        precision=lax.Precision.HIGHEST,
    )

    keep = lax.dynamic_slice_in_dim(right, n * width, width, 1)
    give = lax.dynamic_slice_in_dim(right, (1 - n) * width, width, 1)
    step = [(i, (i + 1) % rows) for i in range(rows)]
    from_low = lax.ppermute(give, "row", step)
    from_high = lax.ppermute(give, "row", [(j, i) for i, j in step])
    from_far = lax.ppermute(keep, "row", [(i, (i + 2) % rows) for i in range(rows)])
    own_b = jnp.concatenate([keep, from_far, from_high, from_low], 0)

    spread = jnp.broadcast_to(picked[None], (cols,) + picked.shape)
    full = lax.all_to_all(spread, "col", split_axis=0, concat_axis=0, tiled=True)
    full = full.reshape(rows, cols // rows * depth, count)

    def ordered(part, at):
        order = [at, at + 2, at + 1, at - 1]
        return jnp.concatenate(
            [lax.dynamic_index_in_dim(part, i % rows, 0, keepdims=False) for i in order],
            0,
        )

    near_a, far_a = full[..., : 2 * close], full[..., 2 * close :]
    near_pair = lax.ppermute(ordered(near_a, x ^ 1), "row", swap_pair)
    far_pair = lax.ppermute(ordered(far_a, x ^ 1), "row", swap_pair)
    near_a, far_a = ordered(near_a, x), ordered(far_a, x)

    def product(a):
        part = dot(a, own_b)
        other = part[close:]
        return part[:close] + lax.ppermute(other, "layer", swap_core)

    part = dot(jnp.concatenate([far_a, far_pair], 1), own_b)
    part = part.reshape(4, distant, width)
    other = jnp.concatenate([part[1], part[3]], 0)
    other = lax.ppermute(other, "layer", swap_core)
    own_far, pair_far = part[0] + other[:distant], part[2] + other[distant:]

    def reduce(near, far_p):
        near_p = product(near)
        total = lax.ppermute(near_p[:height], "layer", onward)
        total = jnp.concatenate(
            [near_p[height : 2 * height] + total, near_p[2 * height :]], 0
        )
        total = lax.ppermute(total, "layer", onward)
        total = lax.ppermute(total + far_p[: 2 * height], "layer", onward)
        total = total + far_p[2 * height : 4 * height]
        return total[:height], total[height:], far_p[4 * height :]

    same, cross, here = reduce(near_a, own_far)
    total = lax.ppermute(jnp.concatenate([same, cross], 0), "layer", onward)
    here = here + total[:height] + lax.ppermute(total[height:], "layer", swap_core)
    same, cross, there = reduce(near_pair, pair_far)
    there = lax.ppermute(there, "row", swap_pair)
    total = jnp.concatenate([same, cross], 0)
    total = lax.ppermute(total, ("layer", "row"), joint(onward))
    there = there + total[:height] + lax.ppermute(total[height:], "layer", swap_core)
    return jnp.concatenate(
        [jnp.where(n == 0, here, there), jnp.where(n == 0, there, here)], 1
    )


def solution(mesh):
    in_specs = (P("row", ("layer", "col")), P(("layer", "row"), "col"))
    out_specs = P(("row", "layer"), "col")
    return jax.shard_map(
        body, mesh=mesh, in_specs=in_specs, out_specs=out_specs, check_vma=False
    )
```
